32 devices in a mesh: dp: 8 (over z, x), mp: 4 (over y, core).
Axes of the slice: x: 2, y: 2, z: 4, core: 2. Of those that a mesh axis runs over, the one named last changes fastest.
Arguments:
- patches: bfloat16 [4096, 2048], P('dp'), may hold values from -6 to 6
- cotangent: bfloat16 [4096, 8192], P('dp', 'mp'), may hold values from -0.09375 to 0.09375
- weight: float32 [2048, 8192], P('dp', 'mp'), may hold values from -0.125 to 0.125
- accum: float32 [2048, 8192], P('dp', 'mp'), may hold values from 0.1 to 4
Outputs:
- new_weight: float32 [2048, 8192], P(('dp', 'mp'))
- new_accum: float32 [2048, 8192], P(('dp', 'mp'))
- weight_copy: bfloat16 [2048, 8192], P(None, 'mp')
The draws below stay inside these ranges and needn't reach their ends.
All inputs are finite; a program needn't handle non-finite values.
Results may differ from the reference program's by a relative error of at most 0.001.
Values may be sent and summed in bfloat16 or wider, within the bound.
A program may use at most 192 MiB of HBM per device.

```python
import math
import jax
import jax.numpy as jnp
from jax import lax

D = 2048
FF = 8192
TOKENS = 4096


def spiked(entries, rng, source, target, blocks, factor):
    def block_of(position):
        return (jnp.arange(entries.shape[position]) // (entries.shape[position] // blocks)).reshape((-1,) + (1,) * (entries.ndim - 1 - position))

    one_side = jax.random.permutation(rng, blocks)[block_of(target)]
    far = (block_of(target) + blocks // 2) % blocks
    return jnp.where((block_of(source) == one_side) | (block_of(source) == far), factor * entries, entries)


def block_levels(rng, dims, shards, low, largest):
    def one(position, parts):
        heights = jax.random.uniform(jax.random.fold_in(jax.random.fold_in(rng, 6), position), (parts,), jnp.float32, low / len(shards), largest / len(shards))
        return jnp.repeat(jnp.exp(heights), dims[position] // parts).reshape((-1,) + (1,) * (len(dims) - position - 1))

    loudness = one(*shards[0])
    for cut in shards[1:]:
        loudness = loudness * one(*cut)
    return loudness


def noise(stream_key, shape, width, bound, shards=(), held_as=jnp.bfloat16):
    result = jax.random.normal(stream_key, shape, jnp.float32) * width
    if len(shards) > 0:
        result = block_levels(stream_key, shape, shards, -0.22, 0.18) * result
    return jnp.clip(result, min=-bound, max=bound).astype(held_as)


def noise_with(rng, extent, spread, bound, pieces, heavy, held_as=jnp.bfloat16):
    values = spread * jax.random.normal(rng, extent, jnp.float32)
    if pieces:
        values = values * block_levels(rng, extent, pieces, -0.22, 0.18)
    return jnp.clip(spiked(values, jax.random.fold_in(rng, 3), *heavy), -bound, bound).astype(held_as)


def setup_inputs(seed: int = 0) -> dict:
    key_of = jax.random.split(jax.random.key(seed), 5)
    return {
        "patches": noise_with(key_of[0], (TOKENS, D), 1.0, 6.0, ((0, 8),), (0, 1, 8, 2.0)),
        "cotangent": noise(key_of[1], (TOKENS, FF), TOKENS ** -0.5, 0.09375, ((0, 8), (1, 4))),
        "weight": noise(key_of[2], (D, FF), D ** -0.5, 0.125, ((0, 8), (1, 4)), jnp.float32),
        "accum": jnp.clip(jnp.exp(math.log(4.0) - 3.6888794 * jax.random.uniform(key_of[3], (D, FF), jnp.float32) ** block_levels(key_of[3], (D, FF), ((0, 8), (1, 4)), -0.2, 0.2)), 0.1, 4.0),
    }


learning_rate = 0.02

def reference(patches, cotangent, weight, accum):
    grad = jnp.dot(patches.T, cotangent, preferred_element_type=jnp.float32)
    new_accum = accum + grad * grad
    new_weight = weight - learning_rate * grad * lax.rsqrt(new_accum)
    weight_copy = new_weight.astype(jnp.bfloat16)
    return (new_weight, new_accum, weight_copy)
```

```python
import functools

import jax
import jax.numpy as jnp
from jax import lax
from jax.experimental import pallas as pl
from jax.experimental.pallas import tpu as pltpu
from jax.sharding import PartitionSpec as P

learning_rate = 0.02
chunks = 8


def kernel(a, b, m, p_ref, t_ref, w_ref, s_ref, ow_ref, os_ref, oc_ref,
           pv, tv, wv, sv, cv, rbuf, sbuf,
           psem, tsem, lsem, rsend, rrecv, csend, crecv, xsend, xrecv, msend, mrecv, osem):
    nc, _, tok, cc = tv.shape
    rows, full = w_ref.shape
    sub = rows // m
    me = lax.axis_index("dp")
    mi = lax.axis_index("mp")
    zi = lax.div(me, b)
    xi = lax.rem(me, b)
    has_left = zi > 0
    has_right = zi < a - 1

    def inner(j):
        return lax.rem(xi + j, b)

    def peer(j):
        return {"dp": zi * b + inner(j)}

    def other(j):
        return lax.rem(mi + j, m)

    left, right = {"dp": me - b}, {"dp": me + b}

    def remote(src, dst, send, recv, device):
        return pltpu.make_async_remote_copy(
            src_ref=src, dst_ref=dst, send_sem=send, recv_sem=recv,
            device_id=device, device_id_type=pl.DeviceIdType.MESH)

    def cols(c):
        return pl.ds(pl.multiple_of(c * cc, cc), cc)

    def block(i):
        return pl.ds(pl.multiple_of(i * rows, rows), rows)

    def own_tokens(c):
        return pltpu.make_async_copy(t_ref.at[:, cols(c)], tv.at[c, xi], lsem.at[0, c])

    def own_weight(c):
        return pltpu.make_async_copy(w_ref.at[:, cols(c)], wv.at[c], lsem.at[1, c])

    def own_accum(c):
        return pltpu.make_async_copy(s_ref.at[:, cols(c)], sv.at[c], lsem.at[2, c])

    def own_features(d):
        return pltpu.make_async_copy(p_ref.at[block(d * b + xi)], pv.at[d, xi], psem.at[2, d, 0])

    def send_tokens(c, j):
        return remote(t_ref.at[:, cols(c)], tv.at[c, xi], tsem.at[0, c, j], tsem.at[1, c, j], peer(j))

    def recv_tokens(c, j):
        return remote(t_ref.at[:, cols(c)], tv.at[c, inner(b - j)], tsem.at[0, c, j], tsem.at[1, c, j], peer(j))

    def send_features(d, j):
        return remote(p_ref.at[block(d * b + inner(j))], pv.at[d, xi], psem.at[0, d, j], psem.at[1, d, j], peer(j))

    def recv_features(d, j):
        return remote(p_ref.at[block(d * b + xi)], pv.at[d, inner(b - j)], psem.at[0, d, j], psem.at[1, d, j], peer(j))

    def pass_sum(side, c, d):
        return remote(sbuf.at[c, d], rbuf.at[side, c, d], rsend.at[c, d], rrecv.at[side, c, d],
                      right if side == 0 else left)

    def region(owner, c):
        return oc_ref.at[block(owner), cols(c)]

    def pass_copy(side, c, h, owner, src=None):
        return remote(region(owner, c) if src is None else src, region(owner, c),
                      csend.at[side, c, h], crecv.at[side, c, h], right if side == 0 else left)

    def share_copy(c, z, j, src=None):
        owner = z * b + xi
        return remote(region(owner, c) if src is None else src, region(owner, c),
                      xsend.at[c, z, j], xrecv.at[c, z, j], peer(j))

    def recv_share(c, z, j):
        spot = region(z * b + inner(b - j), c)
        return remote(spot, spot, xsend.at[c, z, j], xrecv.at[c, z, j], peer(j))

    def flat(c, k, src_dev):
        ref = ow_ref if k == 0 else os_ref
        start = pl.multiple_of(src_dev * full + c * cc, cc)
        return ref.at[:, pl.ds(start, cc)]

    def part(c, k, i):
        v = wv if k == 0 else sv
        return v.at[c, pl.ds(pl.multiple_of(i * sub, sub), sub)]

    def send_flat(c, k, j):
        return remote(part(c, k, other(j)), flat(c, k, mi), msend.at[c, k, j], mrecv.at[c, k, j], {"mp": other(j)})

    def recv_flat(c, k, j):
        return remote(part(c, k, mi), flat(c, k, other(m - j)), msend.at[c, k, j], mrecv.at[c, k, j], {"mp": other(j)})

    def own_flat(c, k):
        return pltpu.make_async_copy(part(c, k, mi), flat(c, k, mi), osem.at[c, k])

    def own_copy(c):
        return pltpu.make_async_copy(cv.at[c], region(me, c), osem.at[c, 2])

    barrier = pltpu.get_barrier_semaphore()

    def greet(device):
        pl.semaphore_signal(barrier, inc=1, device_id=device, device_id_type=pl.DeviceIdType.MESH)

    for d in range(a):
        own_features(d).start()

    @pl.loop(0, nc)
    def _(c):
        own_tokens(c).start()
        own_weight(c).start()
        own_accum(c).start()

    for j in range(1, b):
        greet(peer(j))
    for j in range(1, m):
        greet({"mp": other(j)})
    pl.when(has_left)(lambda: greet(left))
    pl.when(has_right)(lambda: greet(right))
    pl.semaphore_wait(barrier, b - 1 + m - 1 + jnp.minimum(zi, 1) + jnp.minimum(a - 1 - zi, 1))

    for j in range(1, b):
        send_tokens(0, j).start()
    order = []
    for k in range(a):
        for d in (a - 1 - k, k):
            if d not in order:
                order.append(d)
    for d in order:
        for j in range(1, b):
            send_features(d, j).start()

    @pl.loop(1, nc)
    def _(c):
        for j in range(1, b):
            send_tokens(c, j).start()

    def partial(c, d):
        total = jnp.dot(pv[d, 0], tv[c, 0], preferred_element_type=jnp.float32)
        for x in range(1, b):
            total += jnp.dot(pv[d, x], tv[c, x], preferred_element_type=jnp.float32)
        return total

    def stage_sums(c):
        own_tokens(c).wait()
        for j in range(1, b):
            recv_tokens(c, j).wait_recv()

        @pl.when(c == 0)
        def _():
            for d in order:
                own_features(d).wait()
                for j in range(1, b):
                    recv_features(d, j).wait_recv()

        def step(side, d):
            sbuf[c, d] = partial(c, d)

            @pl.when(has_left if side == 0 else has_right)
            def _():
                pass_sum(side, c, d).wait_recv()
                sbuf[c, d] += rbuf[side, c, d]

            pass_sum(side, c, d).start()

        for k in range(a):
            pl.when(a - 1 - k > zi)(functools.partial(step, 0, a - 1 - k))
            pl.when(k < zi)(functools.partial(step, 1, k))

    def stage_update(c):
        own_weight(c).wait()
        own_accum(c).wait()
        sbuf[c, zi] = partial(c, zi)
        for side, there in ((0, has_left), (1, has_right)):
            @pl.when(there)
            def _(side=side):
                pass_sum(side, c, zi).wait_recv()
                sbuf[c, zi] += rbuf[side, c, zi]
        grad = sbuf[c, zi]
        summed = sv[c] + grad * grad
        weight = wv[c] - learning_rate * grad * lax.rsqrt(summed)
        sv[c] = summed
        wv[c] = weight
        cv[c] = weight.astype(cv.dtype)
        pl.when(has_right)(lambda: pass_copy(0, c, 0, me, cv.at[c]).start())
        pl.when(has_left)(lambda: pass_copy(1, c, 0, me, cv.at[c]).start())
        for j in range(1, b):
            share_copy(c, zi, j, cv.at[c]).start()
        own_copy(c).start()
        for k in range(2):
            for j in range(1, m):
                send_flat(c, k, j).start()
            own_flat(c, k).start()

    def stage_forward(h, c):
        def hop(side):
            owner_z = zi - h if side == 0 else zi + h
            owner = owner_z * b + xi
            pass_copy(side, c, h - 1, owner).wait_recv()
            pl.when(has_right if side == 0 else has_left)(
                lambda: pass_copy(side, c, h, owner).start())
            for j in range(1, b):
                share_copy(c, owner_z, j).start()

        pl.when(zi >= h)(functools.partial(hop, 0))
        pl.when(zi + h < a)(functools.partial(hop, 1))

    @pl.loop(0, nc + a)
    def _(i):
        pl.when(i < nc)(lambda: stage_sums(i))
        pl.when((i >= 1) & (i - 1 < nc))(lambda: stage_update(i - 1))
        for h in range(1, a):
            pl.when((i >= 1 + h) & (i - 1 - h < nc))(lambda h=h: stage_forward(h, i - 1 - h))

    for d in range(a):
        for j in range(1, b):
            send_features(d, j).wait_send()

    @pl.loop(0, nc)
    def _(c):
        for j in range(1, b):
            send_tokens(c, j).wait_send()
            for z in range(a):
                share_copy(c, z, j).wait_send()
                recv_share(c, z, j).wait_recv()
        for d in range(a):
            pl.when(d != zi)(lambda d=d: pass_sum(0, c, d).wait_send())
        for h in range(a - 1):
            pl.when((zi >= h) & has_right)(lambda h=h: pass_copy(0, c, h, me).wait_send())
            pl.when((zi + h < a) & has_left)(lambda h=h: pass_copy(1, c, h, me).wait_send())
        own_copy(c).wait()
        for k in range(2):
            for j in range(1, m):
                send_flat(c, k, j).wait_send()
                recv_flat(c, k, j).wait_recv()
            own_flat(c, k).wait()


def shards(n, m, patches, cotangent, weight, accum):
    a = 1
    while a * a < n:
        a *= 2
    b = n // a
    nc = chunks
    tok, dim = patches.shape
    rows, full = weight.shape
    cc = full // nc
    f32, bf16 = jnp.float32, jnp.bfloat16
    dma = pltpu.SemaphoreType.DMA
    flops = 2 * tok * b * a * rows * full
    return pl.pallas_call(
        functools.partial(kernel, a, b, m),
        out_shape=(
            jax.ShapeDtypeStruct((rows // m, full * m), f32),
            jax.ShapeDtypeStruct((rows // m, full * m), f32),
            jax.ShapeDtypeStruct((dim, full), bf16),
        ),
        in_specs=[pl.BlockSpec(memory_space=pl.ANY)] * 4,
        out_specs=(pl.BlockSpec(memory_space=pl.ANY),) * 3,
        scratch_shapes=[
            pltpu.VMEM((a, b, rows, tok), bf16),
            pltpu.VMEM((nc, b, tok, cc), bf16),
            pltpu.VMEM((nc, rows, cc), f32),
            pltpu.VMEM((nc, rows, cc), f32),
            pltpu.VMEM((nc, rows, cc), bf16),
            pltpu.VMEM((2, nc, a, rows, cc), f32),
            pltpu.VMEM((nc, a, rows, cc), f32),
            dma((3, a, b)),
            dma((2, nc, b)),
            dma((3, nc)),
            dma((nc, a)),
            dma((2, nc, a)),
            dma((2, nc, a)),
            dma((2, nc, a)),
            dma((nc, a, b)),
            dma((nc, a, b)),
            dma((nc, 2, m)),
            dma((nc, 2, m)),
            dma((nc, 3)),
        ],
        compiler_params=pltpu.CompilerParams(
            collective_id=0, has_side_effects=True, vmem_limit_bytes=60 * 1024 * 1024),
        cost_estimate=pl.CostEstimate(flops=flops, bytes_accessed=4 * dim * full, transcendentals=rows * full),
    )(patches.T, cotangent, weight, accum)


def solution(mesh):
    return jax.shard_map(
        functools.partial(shards, mesh.shape["dp"], mesh.shape["mp"]),
        mesh=mesh,
        in_specs=(P("dp", None), P("dp", "mp"), P("dp", "mp"), P("dp", "mp")),
        out_specs=(P(("dp", "mp"), None), P(("dp", "mp"), None), P(None, "mp")),
        check_vma=False,
    )
```

```python
import functools

import jax
import jax.numpy as jnp
from jax import lax
from jax.experimental import pallas as pl
from jax.experimental.pallas import tpu as pltpu
from jax.sharding import PartitionSpec as P

learning_rate = 0.02
chunks = 8


def kernel(a, b, m, direct, p_ref, t_ref, w_ref, s_ref, ow_ref, os_ref, oc_ref,
           pv, tv, wv, sv, cv, rbuf, sbuf,
           psem, tsem, lsem, rsend, rrecv, csend, crecv, xsend, xrecv, msend, mrecv, osem):
    nc, _, tok, cc = tv.shape
    rows, full = w_ref.shape
    sub = rows // m
    me = lax.axis_index("dp")
    mi = lax.axis_index("mp")
    zi = lax.div(me, b)
    xi = lax.rem(me, b)
    has_left = zi > 0
    has_right = zi < a - 1

    def inner(j):
        return lax.rem(xi + j, b)

    def peer(j):
        return {"dp": zi * b + inner(j)}

    def other(j):
        return lax.rem(mi + j, m)

    left, right = {"dp": me - b}, {"dp": me + b}

    def remote(src, dst, send, recv, device):
        return pltpu.make_async_remote_copy(
            src_ref=src, dst_ref=dst, send_sem=send, recv_sem=recv,
            device_id=device, device_id_type=pl.DeviceIdType.MESH)

    def cols(c):
        return pl.ds(pl.multiple_of(c * cc, cc), cc)

    def block(i):
        return pl.ds(pl.multiple_of(i * rows, rows), rows)

    def features(i):
        return p_ref.at[:, block(i)] if direct else p_ref.at[block(i)]

    def own_tokens(c):
        return pltpu.make_async_copy(t_ref.at[:, cols(c)], tv.at[c, xi], lsem.at[0, c])

    def own_weight(c):
        return pltpu.make_async_copy(w_ref.at[:, cols(c)], wv.at[c], lsem.at[1, c])

    def own_accum(c):
        return pltpu.make_async_copy(s_ref.at[:, cols(c)], sv.at[c], lsem.at[2, c])

    def own_features(d):
        return pltpu.make_async_copy(features(d * b + xi), pv.at[d, xi], psem.at[2, d, 0])

    def send_tokens(c, j):
        return remote(t_ref.at[:, cols(c)], tv.at[c, xi], tsem.at[0, c, j], tsem.at[1, c, j], peer(j))

    def recv_tokens(c, j):
        return remote(t_ref.at[:, cols(c)], tv.at[c, inner(b - j)], tsem.at[0, c, j], tsem.at[1, c, j], peer(j))

    def send_features(d, j):
        return remote(features(d * b + inner(j)), pv.at[d, xi], psem.at[0, d, j], psem.at[1, d, j], peer(j))

    def recv_features(d, j):
        return remote(features(d * b + xi), pv.at[d, inner(b - j)], psem.at[0, d, j], psem.at[1, d, j], peer(j))

    def pass_sum(side, c, d):
        return remote(sbuf.at[c, d], rbuf.at[side, c, d], rsend.at[c, d], rrecv.at[side, c, d],
                      right if side == 0 else left)

    def region(owner, c):
        return oc_ref.at[block(owner), cols(c)]

    def pass_copy(side, c, h, owner, src=None):
        return remote(region(owner, c) if src is None else src, region(owner, c),
                      csend.at[side, c, h], crecv.at[side, c, h], right if side == 0 else left)

    def share_copy(c, z, j, src=None):
        owner = z * b + xi
        return remote(region(owner, c) if src is None else src, region(owner, c),
                      xsend.at[c, z, j], xrecv.at[c, z, j], peer(j))

    def recv_share(c, z, j):
        spot = region(z * b + inner(b - j), c)
        return remote(spot, spot, xsend.at[c, z, j], xrecv.at[c, z, j], peer(j))

    def flat(c, k, src_dev):
        ref = ow_ref if k == 0 else os_ref
        start = pl.multiple_of(src_dev * full + c * cc, cc)
        return ref.at[:, pl.ds(start, cc)]

    def part(c, k, i):
        v = wv if k == 0 else sv
        return v.at[c, pl.ds(pl.multiple_of(i * sub, sub), sub)]

    def send_flat(c, k, j):
        return remote(part(c, k, other(j)), flat(c, k, mi), msend.at[c, k, j], mrecv.at[c, k, j], {"mp": other(j)})

    def recv_flat(c, k, j):
        return remote(part(c, k, mi), flat(c, k, other(m - j)), msend.at[c, k, j], mrecv.at[c, k, j], {"mp": other(j)})

    def own_flat(c, k):
        return pltpu.make_async_copy(part(c, k, mi), flat(c, k, mi), osem.at[c, k])

    def own_copy(c):
        return pltpu.make_async_copy(cv.at[c], region(me, c), osem.at[c, 2])

    barrier = pltpu.get_barrier_semaphore()

    def greet(device):
        pl.semaphore_signal(barrier, inc=1, device_id=device, device_id_type=pl.DeviceIdType.MESH)

    for d in range(a):
        own_features(d).start()

    @pl.loop(0, nc)
    def _(c):
        own_tokens(c).start()
        own_weight(c).start()
        own_accum(c).start()

    for j in range(1, b):
        greet(peer(j))
    for j in range(1, m):
        greet({"mp": other(j)})
    pl.when(has_left)(lambda: greet(left))
    pl.when(has_right)(lambda: greet(right))
    pl.semaphore_wait(barrier, b - 1 + m - 1 + jnp.minimum(zi, 1) + jnp.minimum(a - 1 - zi, 1))

    for j in range(1, b):
        send_tokens(0, j).start()
    def in_order(do):
        for k in range(a):
            pl.when(a - 1 - k > zi)(functools.partial(do, 0, a - 1 - k))
            pl.when(k < zi)(functools.partial(do, 1, k))

    def start_features(_, d):
        for j in range(1, b):
            send_features(d, j).start()

    in_order(start_features)
    start_features(0, zi)

    @pl.loop(1, nc)
    def _(c):
        for j in range(1, b):
            send_tokens(c, j).start()

    def product(p, t):
        return lax.dot_general(p, t, (((0 if direct else 1,), (0,)), ((), ())), preferred_element_type=jnp.float32)

    def partial(c, d):
        total = product(pv[d, 0], tv[c, 0])
        for x in range(1, b):
            total += product(pv[d, x], tv[c, x])
        return total

    def features_here(d):
        own_features(d).wait()
        for j in range(1, b):
            recv_features(d, j).wait_recv()

    def stage_sums(c):
        own_tokens(c).wait()
        for j in range(1, b):
            recv_tokens(c, j).wait_recv()

        def step(side, d):
            pl.when(c == 0)(lambda: features_here(d))
            sbuf[c, d] = partial(c, d)

            @pl.when(has_left if side == 0 else has_right)
            def _():
                pass_sum(side, c, d).wait_recv()
                sbuf[c, d] += rbuf[side, c, d]

            pass_sum(side, c, d).start()

        in_order(step)

    def stage_update(c):
        pl.when(c == 0)(lambda: features_here(zi))
        own_weight(c).wait()
        own_accum(c).wait()
        sbuf[c, zi] = partial(c, zi)
        for side, there in ((0, has_left), (1, has_right)):
            @pl.when(there)
            def _(side=side):
                pass_sum(side, c, zi).wait_recv()
                sbuf[c, zi] += rbuf[side, c, zi]
        grad = sbuf[c, zi]
        summed = sv[c] + grad * grad
        weight = wv[c] - learning_rate * grad * lax.rsqrt(summed)
        sv[c] = summed
        wv[c] = weight
        cv[c] = weight.astype(cv.dtype)
        pl.when(has_right)(lambda: pass_copy(0, c, 0, me, cv.at[c]).start())
        pl.when(has_left)(lambda: pass_copy(1, c, 0, me, cv.at[c]).start())
        for j in range(1, b):
            share_copy(c, zi, j, cv.at[c]).start()
        own_copy(c).start()
        for k in range(2):
            for j in range(1, m):
                send_flat(c, k, j).start()
            own_flat(c, k).start()

    def stage_forward(h, c):
        def hop(side):
            owner_z = zi - h if side == 0 else zi + h
            owner = owner_z * b + xi
            pass_copy(side, c, h - 1, owner).wait_recv()
            pl.when(has_right if side == 0 else has_left)(
                lambda: pass_copy(side, c, h, owner).start())
            for j in range(1, b):
                share_copy(c, owner_z, j).start()

        pl.when(zi >= h)(functools.partial(hop, 0))
        pl.when(zi + h < a)(functools.partial(hop, 1))

    @pl.loop(0, nc + a)
    def _(i):
        pl.when(i < nc)(lambda: stage_sums(i))
        pl.when((i >= 1) & (i - 1 < nc))(lambda: stage_update(i - 1))
        for h in range(1, a):
            pl.when((i >= 1 + h) & (i - 1 - h < nc))(lambda h=h: stage_forward(h, i - 1 - h))

    for d in range(a):
        for j in range(1, b):
            send_features(d, j).wait_send()

    @pl.loop(0, nc)
    def _(c):
        for j in range(1, b):
            send_tokens(c, j).wait_send()
            for z in range(a):
                share_copy(c, z, j).wait_send()
                recv_share(c, z, j).wait_recv()
        for d in range(a):
            pl.when(d != zi)(lambda d=d: pass_sum(0, c, d).wait_send())
        for h in range(a - 1):
            pl.when((zi >= h) & has_right)(lambda h=h: pass_copy(0, c, h, me).wait_send())
            pl.when((zi + h < a) & has_left)(lambda h=h: pass_copy(1, c, h, me).wait_send())
        own_copy(c).wait()
        for k in range(2):
            for j in range(1, m):
                send_flat(c, k, j).wait_send()
                recv_flat(c, k, j).wait_recv()
            own_flat(c, k).wait()


def shards(n, m, patches, cotangent, weight, accum):
    a = 1
    while a * a < n:
        a *= 2
    b = n // a
    nc = chunks
    direct = weight.shape[0] % 128 == 0
    tok, dim = patches.shape
    rows, full = weight.shape
    cc = full // nc
    f32, bf16 = jnp.float32, jnp.bfloat16
    dma = pltpu.SemaphoreType.DMA
    flops = 2 * tok * b * a * rows * full
    return pl.pallas_call(
        functools.partial(kernel, a, b, m, direct),
        out_shape=(
            pltpu.VMEM((rows // m, full * m), f32),
            pltpu.VMEM((rows // m, full * m), f32),
            pltpu.VMEM((dim, full), bf16),
        ),
        in_specs=[pl.BlockSpec(memory_space=pl.ANY)] * 4,
        out_specs=(pl.BlockSpec(memory_space=pltpu.VMEM),) * 3,
        scratch_shapes=[
            pltpu.VMEM((a, b, tok, rows) if direct else (a, b, rows, tok), bf16),
            pltpu.VMEM((nc, b, tok, cc), bf16),
            pltpu.VMEM((nc, rows, cc), f32),
            pltpu.VMEM((nc, rows, cc), f32),
            pltpu.VMEM((nc, rows, cc), bf16),
            pltpu.VMEM((2, nc, a, rows, cc), f32),
            pltpu.VMEM((nc, a, rows, cc), f32),
            dma((3, a, b)),
            dma((2, nc, b)),
            dma((3, nc)),
            dma((nc, a)),
            dma((2, nc, a)),
            dma((2, nc, a)),
            dma((2, nc, a)),
            dma((nc, a, b)),
            dma((nc, a, b)),
            dma((nc, 2, m)),
            dma((nc, 2, m)),
            dma((nc, 3)),
        ],
        compiler_params=pltpu.CompilerParams(
            collective_id=0, has_side_effects=True, vmem_limit_bytes=42 * 1024 * 1024),
        cost_estimate=pl.CostEstimate(flops=flops, bytes_accessed=4 * dim * full, transcendentals=rows * full),
    )(patches if direct else patches.T, cotangent, weight, accum)


def solution(mesh):
    return jax.shard_map(
        functools.partial(shards, mesh.shape["dp"], mesh.shape["mp"]),
        mesh=mesh,
        in_specs=(P("dp", None), P("dp", "mp"), P("dp", "mp"), P("dp", "mp")),
        out_specs=(P(("dp", "mp"), None), P(("dp", "mp"), None), P(None, "mp")),
        check_vma=False,
    )
```
